16 devices in a mesh: tp: 2 (over z), dp: 8 (over y, x, core).
Axes of the slice: x: 2, y: 2, z: 2, core: 2. Of those that a mesh axis runs over, the one named last changes fastest.
Arguments:
- tokens: int32 [16, 1024], P('dp')
- labels: int32 [16, 1024], P('dp')
- embedding: float32 [50304, 512], P('tp')
- vec_params: float32 [16, 512], replicated
- w_qkv: float32 [2, 512, 1536], P(None, None, 'tp')
- b_qkv: float32 [2, 8, 192], P(None, 'tp')
- w_out: float32 [2, 512, 512], P(None, 'tp')
- w_up: float32 [2, 512, 2048], P(None, None, 'tp')
- b_up: float32 [2, 2048], P(None, 'tp')
- w_down: float32 [2, 2048, 512], P(None, 'tp')
- mom_embedding: float32 [50304, 512], P('tp')
- mom_vec_params: float32 [16, 512], replicated
- mom_w_qkv: float32 [2, 512, 1536], P(None, None, 'tp')
- mom_b_qkv: float32 [2, 8, 192], P(None, 'tp')
- mom_w_out: float32 [2, 512, 512], P(None, 'tp')
- mom_w_up: float32 [2, 512, 2048], P(None, None, 'tp')
- mom_b_up: float32 [2, 2048], P(None, 'tp')
- mom_w_down: float32 [2, 2048, 512], P(None, 'tp')
- vel_embedding: float32 [50304, 512], P('tp')
- vel_vec_params: float32 [16, 512], replicated
- vel_w_qkv: float32 [2, 512, 1536], P(None, None, 'tp')
- vel_b_qkv: float32 [2, 8, 192], P(None, 'tp')
- vel_w_out: float32 [2, 512, 512], P(None, 'tp')
- vel_w_up: float32 [2, 512, 2048], P(None, None, 'tp')
- vel_b_up: float32 [2, 2048], P(None, 'tp')
- vel_w_down: float32 [2, 2048, 512], P(None, 'tp')
Outputs:
- output 1: float32 [], replicated
- output 2: float32 [50304, 512], P('tp')
- output 3: float32 [16, 512], replicated
- output 4: float32 [2, 512, 1536], P(None, None, 'tp')
- output 5: float32 [2, 8, 192], P(None, 'tp')
- output 6: float32 [2, 512, 512], P(None, 'tp')
- output 7: float32 [2, 512, 2048], P(None, None, 'tp')
- output 8: float32 [2, 2048], P(None, 'tp')
- output 9: float32 [2, 2048, 512], P(None, 'tp')
- output 10: float32 [50304, 512], P('tp')
- output 11: float32 [16, 512], replicated
- output 12: float32 [2, 512, 1536], P(None, None, 'tp')
- output 13: float32 [2, 8, 192], P(None, 'tp')
- output 14: float32 [2, 512, 512], P(None, 'tp')
- output 15: float32 [2, 512, 2048], P(None, None, 'tp')
- output 16: float32 [2, 2048], P(None, 'tp')
- output 17: float32 [2, 2048, 512], P(None, 'tp')
- output 18: float32 [50304, 512], P('tp')
- output 19: float32 [16, 512], replicated
- output 20: float32 [2, 512, 1536], P(None, None, 'tp')
- output 21: float32 [2, 8, 192], P(None, 'tp')
- output 22: float32 [2, 512, 512], P(None, 'tp')
- output 23: float32 [2, 512, 2048], P(None, None, 'tp')
- output 24: float32 [2, 2048], P(None, 'tp')
- output 25: float32 [2, 2048, 512], P(None, 'tp')
- output 26: bfloat16 [50304, 512], P('tp')
- output 27: bfloat16 [16, 512], replicated
- output 28: bfloat16 [2, 512, 1536], P(None, None, 'tp')
- output 29: bfloat16 [2, 8, 192], P(None, 'tp')
- output 30: bfloat16 [2, 512, 512], P(None, 'tp')
- output 31: bfloat16 [2, 512, 2048], P(None, None, 'tp')
- output 32: bfloat16 [2, 2048], P(None, 'tp')
- output 33: bfloat16 [2, 2048, 512], P(None, 'tp')
All inputs are finite; a program needn't handle non-finite values.
Results may differ from the reference program's by a relative error of at most 0.001.
Values sent between devices are 32-bit elements.
A program may use at most 1.75 GiB of HBM per device.

```python
import math
import jax
import jax.numpy as jnp
from jax import lax

VOCAB = 50304
D = 512
HEADS = 8
HEAD = 64
LAYERS = 2
SEQ = 1024
BATCH = 16
STEP_COUNT = 10

FF_WIDTH = 4 * D
NUM_VECS = 4 + 6 * LAYERS
LN_EPS = 1e-5
CLIP_NORM = 1.0
BETA_ONE = 0.9
BETA_TWO = 0.95
ADAM_EPS = 1e-8
WEIGHT_DECAY = 0.1
LEARN_RATE = 1e-3
DECAYED = (True, False, True, False, True, True, False, True)
PARAM_NAMES = ('embedding', 'vec_params', 'w_qkv', 'b_qkv', 'w_out', 'w_up', 'b_up', 'w_down')


def alibi_slopes(heads):
    closest = 2 ** int(math.floor(math.log2(heads)))
    first_base = 2.0 ** (-8.0 / closest)
    slopes = [first_base ** (head_idx + 1) for head_idx in range(closest)]
    extra_base = 2.0 ** (-4.0 / closest)
    extra_count = min(closest, heads - closest)
    return slopes + [extra_base ** (2 * head_idx + 1) for head_idx in range(extra_count)]


def layer_norm(values, gain, bias):
    centred = values - jnp.mean(values, axis=-1, keepdims=True)
    variance = jnp.mean(centred * centred, axis=-1, keepdims=True)
    return centred * lax.rsqrt(variance + LN_EPS) * gain + bias


def snap_bf16(values):
    return values + lax.stop_gradient(values.astype(jnp.bfloat16).astype(jnp.float32) - values)


def adam_update(master, grad_arr, moment, velocity, decayed):
    mom_new = BETA_ONE * moment + (1.0 - BETA_ONE) * grad_arr
    vel_new = BETA_TWO * velocity + (1.0 - BETA_TWO) * grad_arr * grad_arr
    mom_hat = mom_new / (1.0 - BETA_ONE ** STEP_COUNT)
    vel_hat = vel_new / (1.0 - BETA_TWO ** STEP_COUNT)
    direction = mom_hat / (jnp.sqrt(vel_hat) + ADAM_EPS)
    if decayed:
        direction = direction + WEIGHT_DECAY * master
    return master - LEARN_RATE * direction, mom_new, vel_new


def seq_loss(params, tok_seq, lab_seq):
    embedding, vec_params, w_qkv, b_qkv, w_out, w_up, b_up, w_down = params
    positions = jnp.arange(SEQ)
    rel_pos = (positions[None, :] - positions[:, None]).astype(jnp.float32)
    causal = positions[None, :] <= positions[:, None]
    slopes = jnp.array(alibi_slopes(HEADS), dtype=jnp.float32)
    emb_snap = snap_bf16(embedding)
    resid = layer_norm(jnp.take(emb_snap, tok_seq, axis=0), vec_params[0], vec_params[1])
    for layer in range(LAYERS):
        row_base = 2 + 6 * layer
        act_in = snap_bf16(layer_norm(resid, vec_params[row_base], vec_params[row_base + 1]))
        qkv = snap_bf16(jnp.dot(act_in, snap_bf16(w_qkv[layer]), preferred_element_type=jnp.float32) + b_qkv[layer].reshape(-1))
        qkv = qkv.reshape(SEQ, HEADS, 3, HEAD)
        scores = jnp.einsum('qhd,khd->hqk', qkv[:, :, 0], qkv[:, :, 1]) * HEAD ** -0.5 + slopes[:, None, None] * rel_pos[None]
        scores = jnp.where(causal[None], scores, -jnp.inf)
        probs = snap_bf16(jax.nn.softmax(scores, axis=-1))
        context = snap_bf16(jnp.einsum('hqk,khd->qhd', probs, qkv[:, :, 2])).reshape(SEQ, D)
        resid = resid + jnp.dot(context, snap_bf16(w_out[layer]), preferred_element_type=jnp.float32) + vec_params[row_base + 2]
        mlp_in = snap_bf16(layer_norm(resid, vec_params[row_base + 3], vec_params[row_base + 4]))
        hidden = snap_bf16(jax.nn.gelu(jnp.dot(mlp_in, snap_bf16(w_up[layer]), preferred_element_type=jnp.float32) + b_up[layer], approximate=True))
        resid = resid + jnp.dot(hidden, snap_bf16(w_down[layer]), preferred_element_type=jnp.float32) + vec_params[row_base + 5]
    final_row = 2 + 6 * LAYERS
    head_in = snap_bf16(layer_norm(resid, vec_params[final_row], vec_params[final_row + 1]))
    logits = jnp.dot(head_in, emb_snap.T, preferred_element_type=jnp.float32)
    target = jnp.take_along_axis(logits, lab_seq[:, None], axis=1)[:, 0]
    return jnp.sum(jax.nn.logsumexp(logits, axis=-1) - target)


def setup_inputs(seed: int = 0) -> dict:
    keys = jax.random.split(jax.random.key(seed), 28)
    tokens = jax.random.randint(keys[0], (BATCH, SEQ), 0, VOCAB, dtype=jnp.int32)
    label_flat = jax.random.randint(keys[1], (BATCH * SEQ,), 0, VOCAB, dtype=jnp.int32)
    spread = jnp.arange(8, dtype=jnp.int32) * (VOCAB // 8) + jax.random.randint(keys[2], (8,), 0, VOCAB // 8, dtype=jnp.int32)
    labels = label_flat.at[:8].set(spread).reshape(BATCH, SEQ)
    row_base = jnp.array([1.0, 0.0] + [1.0, 0.0, 0.0, 1.0, 0.0, 0.0] * LAYERS + [16.0, 0.0], dtype=jnp.float32)
    row_scale = jnp.array([0.2] * (2 + 6 * LAYERS) + [3.2, 0.5], dtype=jnp.float32)
    shapes = [(VOCAB, D), (NUM_VECS, D), (LAYERS, D, 3 * D), (LAYERS, HEADS, 3 * HEAD), (LAYERS, D, D), (LAYERS, D, FF_WIDTH), (LAYERS, FF_WIDTH), (LAYERS, FF_WIDTH, D)]
    scales = [0.2 * D ** -0.5, 1.0, D ** -0.5, 0.2, D ** -0.5, D ** -0.5, 0.2, FF_WIDTH ** -0.5]
    masters = [jax.random.normal(keys[3 + slot], shapes[slot], jnp.float32) * scales[slot] for slot in range(8)]
    masters[1] = row_base[:, None] + row_scale[:, None] * masters[1]
    grad_scale = float(VOCAB * D + NUM_VECS * D + LAYERS * (12 * D * D + 3 * D + FF_WIDTH)) ** -0.5
    moms = [jax.random.normal(keys[11 + slot], shapes[slot], jnp.float32) * grad_scale for slot in range(8)]
    vels = [jax.random.uniform(keys[19 + slot], shapes[slot], jnp.float32, 0.25, 2.0) * grad_scale ** 2 for slot in range(8)]
    result = {'tokens': tokens, 'labels': labels}
    for slot in range(8):
        result[PARAM_NAMES[slot]] = masters[slot]
    for slot in range(8):
        result['mom_' + PARAM_NAMES[slot]] = moms[slot]
    for slot in range(8):
        result['vel_' + PARAM_NAMES[slot]] = vels[slot]
    return result


def reference(tokens, labels, embedding, vec_params, w_qkv, b_qkv, w_out, w_up, b_up, w_down, mom_embedding, mom_vec_params, mom_w_qkv, mom_b_qkv, mom_w_out, mom_w_up, mom_b_up, mom_w_down, vel_embedding, vel_vec_params, vel_w_qkv, vel_b_qkv, vel_w_out, vel_w_up, vel_b_up, vel_w_down):
    masters = (embedding, vec_params, w_qkv, b_qkv, w_out, w_up, b_up, w_down)
    moms = (mom_embedding, mom_vec_params, mom_w_qkv, mom_b_qkv, mom_w_out, mom_w_up, mom_b_up, mom_w_down)
    vels = (vel_embedding, vel_vec_params, vel_w_qkv, vel_b_qkv, vel_w_out, vel_w_up, vel_b_up, vel_w_down)

    def total_loss(params):
        def one_seq(pair):
            return seq_loss(params, pair[0], pair[1])
        per_seq = lax.map(jax.checkpoint(one_seq), (tokens, labels))
        return jnp.sum(per_seq) / (BATCH * SEQ)

    loss, grads = jax.value_and_grad(total_loss)(masters)
    sq_total = sum(jnp.sum(grad_arr * grad_arr) for grad_arr in grads)
    clip_coef = jnp.minimum(1.0, CLIP_NORM / (jnp.sqrt(sq_total) + 1e-6))
    updated = [adam_update(masters[slot], grads[slot] * clip_coef, moms[slot], vels[slot], DECAYED[slot]) for slot in range(8)]
    new_masters = [entry[0] for entry in updated]
    new_moms = [entry[1] for entry in updated]
    new_vels = [entry[2] for entry in updated]
    new_bf16 = [entry.astype(jnp.bfloat16) for entry in new_masters]
    return (loss, *new_masters, *new_moms, *new_vels, *new_bf16)
```

```python
import functools
import math
import jax
import jax.numpy as jnp
from jax import lax
from jax.experimental import pallas as pl
from jax.experimental.pallas import tpu as pltpu
from jax.sharding import PartitionSpec as P

ZERO, ONE, TWO, THREE, FOUR = range(5)
LANES = 128
LN_EPS = 1e-5
CLIP_NORM = 1.0
BETA_ONE = 0.9
BETA_TWO = 0.95
ADAM_EPS = 1e-8
WEIGHT_DECAY = 0.1
LEARN_RATE = 1e-3
STEP_COUNT = 10
DECAYED = (True, False, True, False, True, True, False, True)
PARAM_SPECS = (P('tp', None), P(None, None), P(None, None, 'tp'), P(None, 'tp', None), P(None, 'tp', None), P(None, None, 'tp'), P(None, 'tp'), P(None, 'tp', None))
NT = (((ONE,), (ONE,)), ((), ()))
NN = (((ONE,), (ZERO,)), ((), ()))
TN = (((ZERO,), (ZERO,)), ((), ()))
f32 = jnp.float32
bf16 = jnp.bfloat16
MESH = pl.DeviceIdType.MESH
MIB = TWO ** 20
COST = pl.CostEstimate(flops=10 ** 6, bytes_accessed=10 ** 6, transcendentals=ZERO)


def alibi_slopes(heads):
    closest = TWO ** int(math.floor(math.log2(heads)))
    first_base = 2.0 ** (-8.0 / closest)
    slopes = [first_base ** (head_idx + ONE) for head_idx in range(closest)]
    extra_base = 2.0 ** (-4.0 / closest)
    extra_count = min(closest, heads - closest)
    return slopes + [extra_base ** (TWO * head_idx + ONE) for head_idx in range(extra_count)]


def layer_norm(values, gain, bias):
    centred = values - jnp.mean(values, axis=-ONE, keepdims=True)
    variance = jnp.mean(centred * centred, axis=-ONE, keepdims=True)
    return centred * lax.rsqrt(variance + LN_EPS) * gain + bias


def gelu_tanh(values):
    return jax.nn.gelu(values, approximate=True)


def dot(a, b, dims):
    return lax.dot_general(a, b, dims, preferred_element_type=f32)


def adam_update(master, grad_arr, moment, velocity, decayed):
    mom_new = BETA_ONE * moment + (1.0 - BETA_ONE) * grad_arr
    vel_new = BETA_TWO * velocity + (1.0 - BETA_TWO) * grad_arr * grad_arr
    mom_hat = mom_new / (1.0 - BETA_ONE ** STEP_COUNT)
    vel_hat = vel_new / (1.0 - BETA_TWO ** STEP_COUNT)
    direction = mom_hat / (jnp.sqrt(vel_hat) + ADAM_EPS)
    if decayed:
        direction = direction + WEIGHT_DECAY * master
    return master - LEARN_RATE * direction, mom_new, vel_new


WIDE = 256


def share_plan(shapes):
    plan, at = [], ZERO
    for i, (r, c) in enumerate(shapes):
        for j in range(c // WIDE):
            plan.append((i, at, r, j))
            at += r
    return plan, at


def pack_kernel(pos_ref, *refs):
    ins, out = refs[:-ONE], refs[-ONE]
    plan, _ = share_plan([r.shape[ONE:] for r in ins])
    for i, at, r, j in plan:
        out[at:at + r, :] = ins[i][ZERO, :, j * WIDE:(j + ONE) * WIDE]


def pack_share(pos, ws, layer, ndp):
    blocks = [(w.shape[ONE] // ndp, w.shape[TWO]) for w in ws]
    rows = share_plan(blocks)[ONE]
    return pl.pallas_call(
        pack_kernel,
        grid_spec=pltpu.PrefetchScalarGridSpec(
            num_scalar_prefetch=ONE, grid=(ONE,),
            in_specs=[pl.BlockSpec((ONE,) + b, lambda i, p: (layer, p[ZERO], ZERO)) for b in blocks],
            out_specs=pl.BlockSpec((rows, WIDE), lambda i, p: (ZERO, ZERO))),
        out_shape=jax.ShapeDtypeStruct((rows, WIDE), f32),
        cost_estimate=COST,
        name="pack_share")(pos, *ws)


def join_kernel(oth_ref, *refs, hd):
    own, (wd, wu, wo, wq) = refs[:FOUR], refs[FOUR:]
    plan, _ = share_plan([r.shape[ONE:] for r in own])
    oth = [jnp.concatenate([oth_ref[ZERO, at:at + r, :] for i, at, r, j in plan if i == k], axis=ONE) for k in range(FOUR)]
    wd[ZERO], wd[ONE] = own[ZERO][ZERO].astype(bf16), oth[ZERO].astype(bf16)
    wo[ZERO], wo[ONE] = own[TWO][ZERO].astype(bf16), oth[TWO].astype(bf16)
    c = own[ONE].shape[TWO]
    wu[:, :c], wu[:, c:] = own[ONE][ZERO].astype(bf16), oth[ONE].astype(bf16)
    mine, heads = own[THREE][ZERO], own[THREE].shape[TWO] // (THREE * hd)
    for kind in range(THREE):
        cols = [src[:, (THREE * h + kind) * hd:(THREE * h + kind + ONE) * hd] for src in (mine, oth[THREE]) for h in range(heads)]
        width = TWO * heads * hd
        wq[:, kind * width:(kind + ONE) * width] = jnp.concatenate(cols, axis=ONE).astype(bf16)


def join_halves(oth, ws, layer, hd):
    ndp, rows, _ = oth.shape
    blocks = [(w.shape[ONE] // ndp, w.shape[TWO]) for w in ws]
    d, u, o, q = [(w.shape[ONE], w.shape[TWO]) for w in ws]
    stacked = lambda b: pl.BlockSpec((TWO,) + b, lambda p: (ZERO, p, ZERO))
    wide = lambda b: pl.BlockSpec((b[ZERO], TWO * b[ONE]), lambda p: (p, ZERO))
    wd, wu, wo, wq = pl.pallas_call(
        functools.partial(join_kernel, hd=hd), grid=(ndp,),
        in_specs=[pl.BlockSpec((ONE, rows, WIDE), lambda p: (p, ZERO, ZERO))] + [pl.BlockSpec((ONE,) + b, lambda p: (layer, p, ZERO)) for b in blocks],
        out_specs=[stacked(blocks[ZERO]), wide(blocks[ONE]), stacked(blocks[TWO]), wide(blocks[THREE])],
        out_shape=[jax.ShapeDtypeStruct(x, bf16) for x in ((TWO,) + d, (u[ZERO], TWO * u[ONE]), (TWO,) + o, (q[ZERO], TWO * q[ONE]))],
        compiler_params=pltpu.CompilerParams(dimension_semantics=("arbitrary",), vmem_limit_bytes=32 * MIB),
        cost_estimate=COST,
        name="join_halves")(oth, *ws)
    return wd.reshape(TWO * d[ZERO], d[ONE]), wu, wo.reshape(TWO * o[ZERO], o[ONE]), wq


def wgrad_mlp_kernel(z_ref, hid, d_out, mlp_in, d_pre, out):
    ndp = out.shape[ONE]
    g = dot(hid[:], d_out[:], TN)
    r, at = g.shape[ZERO] // ndp, ZERO
    for j in range(g.shape[ONE] // WIDE):
        for p in range(ndp):
            out[ZERO, p, at:at + r, :] = g[p * r:(p + ONE) * r, j * WIDE:(j + ONE) * WIDE]
        at += r
    g = dot(mlp_in[:], d_pre[:], TN)
    r = g.shape[ZERO] // ndp
    for j in range(g.shape[ONE] // WIDE):
        for p in range(ndp):
            out[ZERO, p, at:at + r, :] = g[p * r:(p + ONE) * r, j * WIDE:(j + ONE) * WIDE]
        at += r


def wgrad_attn_kernel(z_ref, ctx, d_attn, act_in, d_q, d_k, d_v, prev, out):
    ndp = out.shape[ONE]
    g = dot(ctx[:], d_attn[:], TN)
    r, at = g.shape[ZERO] // ndp, ZERO
    for j in range(g.shape[ONE] // WIDE):
        for p in range(ndp):
            out[ZERO, p, at:at + r, :] = g[p * r:(p + ONE) * r, j * WIDE:(j + ONE) * WIDE]
        at += r
    for part in (d_q, d_k, d_v):
        g = dot(act_in[:], part[:], TN)
        r = g.shape[ZERO] // ndp
        for j in range(g.shape[ONE] // WIDE):
            for p in range(ndp):
                out[ZERO, p, at:at + r, :] = g[p * r:(p + ONE) * r, j * WIDE:(j + ONE) * WIDE]
            at += r


def wgrad(kernel, z, split, ops, ndp, rows, first, total, prev):
    tok = ops[ZERO].shape[ZERO]
    specs = [pl.BlockSpec((tok, op.shape[ONE] // TWO), lambda i, zr: (ZERO, i)) if cut else pl.BlockSpec(op.shape, lambda i, zr: (ZERO, ZERO)) for op, cut in zip(ops, split)]
    aliases, extra = {}, []
    if prev is not None:
        aliases, extra = {ONE + len(ops): ZERO}, [prev]
        specs.append(pl.BlockSpec(memory_space=pl.ANY))
    return pl.pallas_call(
        kernel,
        grid_spec=pltpu.PrefetchScalarGridSpec(
            num_scalar_prefetch=ONE, grid=(TWO,), in_specs=specs,
            out_specs=pl.BlockSpec((ONE, ndp, rows, WIDE), lambda i, zr: (lax.rem(i + zr[ZERO], TWO), ZERO, first // rows, ZERO))),
        out_shape=jax.ShapeDtypeStruct((TWO, ndp, total, WIDE), f32),
        input_output_aliases=aliases,
        compiler_params=pltpu.CompilerParams(dimension_semantics=("arbitrary",), vmem_limit_bytes=48 * MIB),
        cost_estimate=COST)(z, *ops, *extra)


def adam_layers_kernel(clip_ref, g_ref, *refs, hd):
    states, outs = refs[:12], refs[12:]
    shapes = [r.shape[ONE:] for r in states[:FOUR]]
    plan, _ = share_plan(shapes)
    for k in range(FOUR):
        parts = [g_ref[ZERO, at:at + r, :] for i, at, r, j in plan if i == k]
        if k == THREE:
            heads = shapes[THREE][ONE] // (THREE * hd)
            parts = [parts[kind][:, h * hd:(h + ONE) * hd] for h in range(heads) for kind in range(THREE)]
        g = jnp.concatenate(parts, axis=ONE) * clip_ref[ZERO]
        new, mom, vel = adam_update(states[k][ZERO], g, states[FOUR + k][ZERO], states[8 + k][ZERO], True)
        outs[k][ZERO], outs[FOUR + k][ZERO], outs[8 + k][ZERO], outs[12 + k][ZERO] = new, mom, vel, new.astype(bf16)


def adam_layers(clip, g, ws, ms, vs, layers, hd):
    ndp = g.shape[ZERO]
    rows = g.shape[ONE] // layers
    blocks = [pl.BlockSpec((ONE, w.shape[ONE] // ndp, w.shape[TWO]), lambda la, p: (la, p, ZERO)) for w in ws]
    shapes = [jax.ShapeDtypeStruct(w.shape, f32) for w in ws]
    return pl.pallas_call(
        functools.partial(adam_layers_kernel, hd=hd), grid=(layers, ndp),
        in_specs=[pl.BlockSpec(memory_space=pltpu.SMEM), pl.BlockSpec((ONE, rows, WIDE), lambda la, p: (p, la, ZERO))] + blocks * THREE,
        out_specs=blocks * FOUR,
        out_shape=shapes * THREE + [jax.ShapeDtypeStruct(w.shape, bf16) for w in ws],
        compiler_params=pltpu.CompilerParams(dimension_semantics=("arbitrary", "arbitrary"), vmem_limit_bytes=40 * MIB),
        cost_estimate=COST,
        name="adam_layers")(clip, g, *ws, *ms, *vs)


def gather_kernel(ids_ref, emb, out, buf, sem):
    n = out.shape[ZERO]

    def go(i, carry):
        pltpu.make_async_copy(emb.at[pl.ds(ids_ref[i], ONE)], buf.at[pl.ds(i, ONE)], sem).start()
        return carry

    lax.fori_loop(ZERO, n, go, ZERO, unroll=16)
    pltpu.make_async_copy(emb.at[pl.ds(ZERO, n)], buf, sem).wait()
    out[:] = buf[:].astype(bf16).astype(f32)


def gather_rows(ids, emb):
    n, dim = ids.shape[ZERO], emb.shape[ONE]
    return pl.pallas_call(
        gather_kernel, in_specs=[pl.BlockSpec(memory_space=pltpu.SMEM), pl.BlockSpec(memory_space=pl.ANY)],
        out_specs=pl.BlockSpec(memory_space=pltpu.VMEM), out_shape=jax.ShapeDtypeStruct((n, dim), f32),
        scratch_shapes=[pltpu.VMEM((n, dim), f32), pltpu.SemaphoreType.DMA],
        compiler_params=pltpu.CompilerParams(vmem_limit_bytes=20 * MIB),
        cost_estimate=COST,
        name="gather_rows")(ids, emb)


def slab_kernel(idx_ref, emb, out, buf, sems):
    _, live, dim = buf.shape
    half = out.shape[ZERO] // TWO
    copies = [pltpu.make_async_copy(emb.at[pl.ds(pl.multiple_of(idx_ref[i] * live, 8), live)], buf.at[i], sems.at[i]) for i in range(TWO)]
    for copy in copies:
        copy.start()
    for i, copy in enumerate(copies):
        copy.wait()
        out[i * half:i * half + live, :] = buf[i].astype(bf16)
        out[i * half + live:(i + ONE) * half, :] = jnp.zeros((half - live, dim), bf16)


def make_slab(idx, emb, live, half):
    dim = emb.shape[ONE]
    return pl.pallas_call(
        slab_kernel, in_specs=[pl.BlockSpec(memory_space=pltpu.SMEM), pl.BlockSpec(memory_space=pl.ANY)],
        out_specs=pl.BlockSpec(memory_space=pltpu.VMEM), out_shape=jax.ShapeDtypeStruct((TWO * half, dim), bf16),
        scratch_shapes=[pltpu.VMEM((TWO, live, dim), f32), pltpu.SemaphoreType.DMA((TWO,))],
        compiler_params=pltpu.CompilerParams(vmem_limit_bytes=32 * MIB),
        cost_estimate=COST,
        name="make_slab")(idx, emb)


def attn_probs(k, q, slope, row0, tri):
    kv, blk = k.shape[ZERO], q.shape[ZERO]
    jpos = lax.broadcasted_iota(jnp.int32, (kv, ONE), ZERO).astype(f32)
    s = dot(k, q, NT) + slope * (jpos - float(row0))
    diag = jnp.where(tri, s[kv - blk:, :], -jnp.inf)
    s = diag if kv == blk else jnp.concatenate([s[:kv - blk, :], diag], axis=ZERO)
    e = jnp.exp(s - jnp.max(s, axis=ZERO, keepdims=True))
    return e * (1.0 / jnp.sum(e, axis=ZERO, keepdims=True))


def attn_fwd_kernel(slope_ref, q_ref, k_ref, v_ref, o_ref, *, blk, hd):
    pair = pl.program_id(ZERO)
    lane = lax.broadcasted_iota(jnp.int32, (ONE, TWO * hd), ONE)
    tri = lax.broadcasted_iota(jnp.int32, (blk, blk), ZERO) <= lax.broadcasted_iota(jnp.int32, (blk, blk), ONE)
    for i in reversed(range(q_ref.shape[ZERO] // blk)):
        kv = (i + ONE) * blk
        q, k, v = q_ref[i * blk:kv, :], k_ref[:kv, :], v_ref[:kv, :]
        outs = []
        for a in range(TWO):
            sel = (lane >= hd) if a else (lane < hd)
            qa = jnp.where(sel, q, jnp.zeros_like(q)) * jnp.asarray(hd ** -0.5, bf16)
            p = attn_probs(k, qa, slope_ref[TWO * pair + a], i * blk, tri)
            outs.append(dot(p.astype(bf16), v, TN))
        o_ref[i * blk:kv, :] = jnp.where(lane < hd, outs[ZERO], outs[ONE]).astype(bf16)


def attn_bwd_kernel(slope_ref, q_ref, k_ref, v_ref, do_ref, dq_ref, dk_ref, dv_ref, db_ref, dkacc, dvacc, *, blk, hd):
    pair = pl.program_id(ZERO)
    n = q_ref.shape[ZERO] // blk
    scale = hd ** -0.5
    lane = lax.broadcasted_iota(jnp.int32, (ONE, TWO * hd), ONE)
    tri = lax.broadcasted_iota(jnp.int32, (blk, blk), ZERO) <= lax.broadcasted_iota(jnp.int32, (blk, blk), ONE)
    qsum = jnp.zeros((ONE, TWO * hd), f32)
    for i in reversed(range(n)):
        kv = (i + ONE) * blk
        q, do = q_ref[i * blk:kv, :], do_ref[i * blk:kv, :]
        k, v = k_ref[:kv, :], v_ref[:kv, :]
        dqs, dks, dvs = [], [], []
        for a in range(TWO):
            sel = (lane >= hd) if a else (lane < hd)
            qs = jnp.where(sel, q, jnp.zeros_like(q))
            doa = jnp.where(sel, do, jnp.zeros_like(do))
            p = attn_probs(k, qs * jnp.asarray(scale, bf16), slope_ref[TWO * pair + a], i * blk, tri)
            pdp = p * dot(v, doa, NT)
            delta = jnp.sum(pdp, axis=ZERO, keepdims=True)
            ds = ((pdp - p * delta) * scale).astype(bf16)
            dvs.append(dot(p.astype(bf16), doa, NN))
            dks.append(dot(ds, qs, NN))
            dqs.append(dot(ds, k, TN))
        dq = jnp.where(lane < hd, dqs[ZERO], dqs[ONE])
        qsum = qsum + jnp.sum(dq, axis=ZERO, keepdims=True)
        dq_ref[i * blk:kv, :] = dq.astype(bf16)
        if i == n - ONE:
            dkacc[:] = dks[ZERO] + dks[ONE]
            dvacc[:] = dvs[ZERO] + dvs[ONE]
        else:
            dkacc[:kv, :] += dks[ZERO] + dks[ONE]
            dvacc[:kv, :] += dvs[ZERO] + dvs[ONE]
    dk_ref[:] = dkacc[:].astype(bf16)
    dv_ref[:] = dvacc[:].astype(bf16)
    db_ref[ZERO:ONE, :] = qsum
    db_ref[ONE:TWO, :] = jnp.sum(dkacc[:], axis=ZERO, keepdims=True)
    db_ref[TWO:THREE, :] = jnp.sum(dvacc[:], axis=ZERO, keepdims=True)
    db_ref[THREE:8, :] = jnp.zeros((5, TWO * hd), f32)


def attn_fwd(qkv, slopes, hd, blk):
    seq, width = qkv.shape
    dim = width // THREE
    npair = dim // (TWO * hd)
    spec = lambda off: pl.BlockSpec((seq, TWO * hd), lambda h: (ZERO, h + off))
    return pl.pallas_call(
        functools.partial(attn_fwd_kernel, blk=blk, hd=hd), grid=(npair,),
        in_specs=[pl.BlockSpec(memory_space=pltpu.SMEM), spec(ZERO), spec(npair), spec(TWO * npair)],
        out_specs=spec(ZERO), out_shape=jax.ShapeDtypeStruct((seq, dim), bf16),
        compiler_params=pltpu.CompilerParams(dimension_semantics=("arbitrary",), vmem_limit_bytes=40 * MIB),
        cost_estimate=COST,
        name="attn_fwd")(slopes, qkv, qkv, qkv)


def attn_bwd(qkv, d_ctx, slopes, hd, blk):
    seq, width = qkv.shape
    dim = width // THREE
    npair = dim // (TWO * hd)
    spec = lambda off: pl.BlockSpec((seq, TWO * hd), lambda h: (ZERO, h + off))
    return pl.pallas_call(
        functools.partial(attn_bwd_kernel, blk=blk, hd=hd), grid=(npair,),
        in_specs=[pl.BlockSpec(memory_space=pltpu.SMEM), spec(ZERO), spec(npair), spec(TWO * npair), spec(ZERO)],
        out_specs=[spec(ZERO)] * THREE + [pl.BlockSpec((8, TWO * hd), lambda h: (ZERO, h))],
        out_shape=[jax.ShapeDtypeStruct((seq, dim), bf16)] * THREE + [jax.ShapeDtypeStruct((8, dim), f32)],
        scratch_shapes=[pltpu.VMEM((seq, TWO * hd), f32)] * TWO,
        compiler_params=pltpu.CompilerParams(dimension_semantics=("arbitrary",), vmem_limit_bytes=48 * MIB),
        cost_estimate=COST,
        name="attn_bwd")(slopes, qkv, qkv, qkv, d_ctx)


def head_fwd_kernel(*refs, npiece, nself, vb, half, live):
    e_ref, h_refs = refs[ZERO], refs[ONE:ONE + npiece]
    m_ref, s_ref, hb_ref, hs, la, lb, acc = refs[-7:]
    sums = refs[-8 - (ZERO < nself < npiece):-7]
    step = pl.program_id(ZERO)
    nvoc, nb = e_ref.shape[ZERO], e_ref.shape[ZERO] // vb
    for i in range(npiece):
        @pl.when(step == i)
        def _(i=i):
            hs[:] = h_refs[i][:].astype(bf16)
    h = hs[:]
    hb_ref[:] = h
    bufs = (la, lb)

    def logits(b):
        bufs[b % TWO][:] = dot(h, e_ref[b * vb:(b + ONE) * vb, :], NT)

    def drop_padding(b):
        buf = bufs[b % TWO]
        for hh in range(nvoc // half):
            lo, hi = max(hh * half + live - b * vb, ZERO), min((hh + ONE) * half - b * vb, vb)
            if lo < hi:
                a0, a1 = lo // LANES * LANES, -(-hi // LANES) * LANES
                col = lax.broadcasted_iota(jnp.int32, (ONE, a1 - a0), ONE) + a0
                buf[:, a0:a1] = jnp.where((col >= lo) & (col < hi), -jnp.inf, buf[:, a0:a1])

    top = total = None
    logits(ZERO)
    for b in range(nb):
        if b + ONE < nb:
            logits(b + ONE)
        drop_padding(b)
        lg = bufs[b % TWO][:]
        e = e_ref[b * vb:(b + ONE) * vb, :]
        blk_top = jnp.max(lg, axis=ONE, keepdims=True)
        if b == ZERO:
            top = blk_top
            p = jnp.exp(lg - top)
            total = jnp.sum(p, axis=ONE, keepdims=True)
            acc[:] = dot(p.astype(bf16), e, NN)
        else:
            new = jnp.maximum(top, blk_top)
            alpha = jnp.exp(top - new)
            p = jnp.exp(lg - new)
            total = total * alpha + jnp.sum(p, axis=ONE, keepdims=True)
            acc[:] = acc[:] * alpha + dot(p.astype(bf16), e, NN)
            top = new
    m_ref[:] = jnp.transpose(top)[None]
    s_ref[:] = jnp.transpose(total)[None]

    if len(sums) == ONE:
        sums[ZERO][:] = acc[:]
    else:
        @pl.when(step < nself)
        def _():
            sums[ZERO][:] = acc[:]

        @pl.when(step >= nself)
        def _():
            sums[ONE][:] = acc[:]


def head_fwd(slab, self_pieces, core_pieces, hb, pos, total_pieces, t, live, vb):
    pieces = list(self_pieces) + list(core_pieces)
    n, k = len(pieces), len(self_pieces)
    nvoc, dim = slab.shape
    ins = [slab] + [arr for arr, _ in pieces]
    in_specs = [pl.BlockSpec((nvoc, dim), lambda i: (ZERO, ZERO))] + [pl.BlockSpec((t, dim), lambda i, blk=blk: (blk, ZERO)) for _, blk in pieces]
    row = pl.BlockSpec((ONE, ONE, t), lambda i: (i, ZERO, ZERO))
    out_specs, out_shape = [], []
    if k:
        out_specs.append(pl.BlockSpec((t, dim), lambda i: (jnp.minimum(i, k - ONE), ZERO)))
        out_shape.append(jax.ShapeDtypeStruct((k * t, dim), f32))
    if n > k:
        out_specs.append(pl.BlockSpec((t, dim), lambda i: (jnp.maximum(i - k, ZERO), ZERO)))
        out_shape.append(jax.ShapeDtypeStruct(((n - k) * t, dim), f32))
    out_specs += [row, row, pl.BlockSpec((t, dim), lambda i: (i + pos, ZERO))]
    stats = jax.ShapeDtypeStruct((n, ONE, t), f32)
    out_shape += [stats, stats, jax.ShapeDtypeStruct((total_pieces * t, dim), bf16)]
    aliases = {}
    if hb is not None:
        aliases = {len(ins): len(out_shape) - ONE}
        ins.append(hb)
        in_specs.append(pl.BlockSpec(memory_space=pl.ANY))
    return pl.pallas_call(
        functools.partial(head_fwd_kernel, npiece=n, nself=k, vb=vb, half=nvoc // TWO, live=live), grid=(n,),
        in_specs=in_specs, out_specs=out_specs, out_shape=out_shape,
        scratch_shapes=[pltpu.VMEM((t, dim), bf16), pltpu.VMEM((t, vb), f32), pltpu.VMEM((t, vb), f32), pltpu.VMEM((t, dim), f32)],
        input_output_aliases=aliases,
        compiler_params=pltpu.CompilerParams(dimension_semantics=("arbitrary",), vmem_limit_bytes=58 * MIB),
        cost_estimate=COST,
        name="head_fwd")(*ins)


def head_grad_kernel(base_ref, e_ref, h_ref, lse_ref, lab_ref, g_ref, *, tt, sub, inv):
    vb = e_ref.shape[ZERO]
    base = base_ref[ZERO] + pl.program_id(ZERO) * vb

    def step(t, carry):
        h = h_ref[pl.ds(pl.multiple_of(t * tt, tt), tt), :]
        lse, lab = lse_ref[t], lab_ref[t]
        for r in range(vb // sub):
            row = lax.broadcasted_iota(jnp.int32, (sub, ONE), ZERO) + (base + r * sub)
            p = jnp.exp(dot(e_ref[r * sub:(r + ONE) * sub, :], h, NT) - lse)
            d = jnp.where(row == lab, p - 1.0, p).astype(bf16)
            g_ref[r * sub:(r + ONE) * sub, :] += dot(d, h, NN)
        return carry

    g_ref[:] = jnp.zeros_like(g_ref)
    lax.fori_loop(ZERO, h_ref.shape[ZERO] // tt, step, ZERO)
    g_ref[:] *= inv


def head_grad(base, slab, first_block, nblocks, h, lse, lab, vb, tt, sub, inv):
    ntok, dim = h.shape
    n = ntok // tt
    return pl.pallas_call(
        functools.partial(head_grad_kernel, tt=tt, sub=sub, inv=inv), grid=(nblocks,),
        in_specs=[pl.BlockSpec(memory_space=pltpu.SMEM), pl.BlockSpec((vb, dim), lambda b: (b + first_block, ZERO)),
                  pl.BlockSpec((ntok, dim), lambda b: (ZERO, ZERO)),
                  pl.BlockSpec((n, ONE, tt), lambda b: (ZERO, ZERO, ZERO)), pl.BlockSpec((n, ONE, tt), lambda b: (ZERO, ZERO, ZERO))],
        out_specs=pl.BlockSpec((vb, dim), lambda b: (b, ZERO)),
        out_shape=jax.ShapeDtypeStruct((nblocks * vb, dim), f32),
        compiler_params=pltpu.CompilerParams(dimension_semantics=("arbitrary",), vmem_limit_bytes=58 * MIB),
        cost_estimate=COST,
        name="head_grad")(base, slab, h, lse, lab)


def scatter_kernel(count_ref, key_ref, d_hbm, *refs, chunk, depth, ring, nin, rows):
    own_refs, g_refs, (*g_outs, sq_ref, acc, buf, sems) = refs[:nin], refs[nin:TWO * nin], refs[TWO * nin:]
    n = count_ref[ZERO]
    acc[:] = jnp.zeros_like(acc)
    nchunk = (n + chunk - ONE) // chunk

    def fetch(c):
        slot = c % ring

        def one(i, carry):
            pltpu.make_async_copy(d_hbm.at[key_ref[c * chunk + i] // depth], buf.at[slot, i], sems.at[slot]).start()
            return carry

        lax.fori_loop(ZERO, chunk, one, ZERO, unroll=16)

    for c in range(ring - ONE):
        @pl.when(c < nchunk)
        def _(c=c):
            fetch(c)

    def body(c, carry):
        @pl.when(c + ring - ONE < nchunk)
        def _():
            fetch(c + ring - ONE)

        slot = c % ring
        pltpu.make_async_copy(d_hbm.at[pl.ds(ZERO, chunk)], buf.at[slot], sems.at[slot]).wait()

        def add(i, carry):
            acc[key_ref[c * chunk + i] % depth] += buf[slot, i]
            return carry

        lax.fori_loop(ZERO, chunk, add, ZERO, unroll=16)
        return carry

    lax.fori_loop(ZERO, nchunk, body, ZERO)
    sq = jnp.zeros((8, LANES), f32)
    for j in range(FOUR):
        done = ZERO
        for part, g_ref in enumerate(g_refs):
            take = min(g_ref.shape[ZERO], rows - done)
            cols = slice(j * LANES, (j + ONE) * LANES)
            val = own_refs[part][:take, cols] + g_ref[:take, cols] + acc[pl.ds(done, take), j, :]
            g_outs[j // TWO][done:done + take, (j % TWO) * LANES:(j % TWO + ONE) * LANES] = val
            sq = sq + jnp.sum((val * val).reshape(take // 8, 8, LANES), axis=ZERO)
            done += take
    sq_ref[:] = sq


def add_lookup_rows(count, keys, d_all, own, grads, rows, depth, chunk=64, ring=FOUR):
    vm = pl.BlockSpec(memory_space=pltpu.VMEM)
    sm = pl.BlockSpec(memory_space=pltpu.SMEM)
    dim = grads[ZERO].shape[ONE]
    return pl.pallas_call(
        functools.partial(scatter_kernel, chunk=chunk, depth=depth, ring=ring, nin=len(grads), rows=rows),
        in_specs=[sm, sm, pl.BlockSpec(memory_space=pl.ANY)] + [vm] * TWO * len(grads),
        out_specs=[vm, vm, vm],
        out_shape=[jax.ShapeDtypeStruct((rows, dim // TWO), f32), jax.ShapeDtypeStruct((rows, dim // TWO), f32), jax.ShapeDtypeStruct((8, LANES), f32)],
        scratch_shapes=[pltpu.VMEM((rows + 8, FOUR, LANES), f32), pltpu.VMEM((ring, chunk, FOUR, LANES), f32), pltpu.SemaphoreType.DMA((ring,))],
        compiler_params=pltpu.CompilerParams(vmem_limit_bytes=58 * MIB),
        cost_estimate=COST,
        name="lookup_rows")(count, keys, d_all, *own, *grads)


def small_sum_kernel(x_ref, o_ref, slots, send_sem, recv_sem, *, ntp, ndp):
    tp, dp = lax.axis_index('tp'), lax.axis_index('dp')
    me = tp * ndp + dp
    n = ntp * ndp
    barrier = pltpu.get_barrier_semaphore()
    peers = [(lax.rem(tp + k // ndp, ntp), lax.rem(dp + k % ndp, ndp)) for k in range(ONE, n)]
    for peer in peers:
        pl.semaphore_signal(barrier, inc=ONE, device_id=peer, device_id_type=MESH)
    pl.semaphore_wait(barrier, n - ONE)
    copies = []
    for k, peer in enumerate(peers):
        copies.append(pltpu.make_async_remote_copy(src_ref=x_ref, dst_ref=slots.at[me], send_sem=send_sem.at[k], recv_sem=recv_sem.at[k], device_id=peer, device_id_type=MESH))
        copies[-ONE].start()
    slots[me] = x_ref[:]
    for copy in copies:
        copy.wait()
    total = slots[ZERO]
    for k in range(ONE, n):
        total = total + slots[k]
    o_ref[:] = total


def small_sum(x, ntp, ndp, cid):
    vm = pl.BlockSpec(memory_space=pltpu.VMEM)
    n = ntp * ndp
    return pl.pallas_call(
        functools.partial(small_sum_kernel, ntp=ntp, ndp=ndp), in_specs=[vm], out_specs=vm,
        out_shape=jax.ShapeDtypeStruct(x.shape, f32),
        scratch_shapes=[pltpu.VMEM((n,) + x.shape, f32), pltpu.SemaphoreType.DMA((n - ONE,)), pltpu.SemaphoreType.DMA((n - ONE,))],
        compiler_params=pltpu.CompilerParams(collective_id=cid, has_side_effects=True),
        cost_estimate=COST)(x)


def grad_sum_kernel(*refs, nl, third, ntp, ndp, live, tt, sub, inv, row0):
    packs, x_ref, slab_ref, h_ref, lse_ref, lab_ref = refs[:nl], *refs[nl:nl + 5]
    out, small_out, g_ref, acc, r_core, r_one, r_two, r_last, slots, s_own, s_core, r_core_s, s_ring, r_ring, s_small, r_small, e_ref, s_slab = refs[nl + 5:]
    tp, dp = lax.axis_index('tp'), lax.axis_index('dp')
    me, n = tp * ndp + dp, ntp * ndp
    core, xx, yy = lax.rem(dp, TWO), lax.rem(dp // TWO, TWO), dp // FOUR
    near = {'core': (tp, dp + ONE - TWO * core), 'x': (tp, dp + TWO - FOUR * xx), 'y': (tp, dp + FOUR - 8 * yy), 'z': (ONE - tp, dp)}
    bit = {'x': xx, 'y': yy, 'z': tp}
    barrier = pltpu.get_barrier_semaphore()
    peers = [(lax.rem(tp + k // ndp, ntp), lax.rem(dp + k % ndp, ndp)) for k in range(ONE, n)]
    for peer in peers:
        pl.semaphore_signal(barrier, inc=ONE, device_id=peer, device_id_type=MESH)
    pl.semaphore_wait(barrier, n - ONE)

    def remote(src, dst, send, recv, peer):
        return pltpu.make_async_remote_copy(src_ref=src, dst_ref=dst, send_sem=send, recv_sem=recv, device_id=peer, device_id_type=MESH)

    over_core, own, small = {}, {}, []
    for k in range(THREE):
        for la in range(nl):
            rows = pl.ds(k * third, third)
            over_core[k, la] = remote(packs[la].at[:, ONE - core, rows, :], r_core.at[k, la], s_core.at[k, la], r_core_s.at[k, la], near['core'])
            over_core[k, la].start()
            own[k, la] = pltpu.make_async_copy(packs[la].at[:, core, rows, :], acc.at[k, la], s_own.at[k, la])
            own[k, la].start()
    for k, peer in enumerate(peers):
        small.append(remote(x_ref, slots.at[me], s_small.at[k], r_small.at[k], peer))
        small[-ONE].start()
    slots[me] = x_ref[:]

    orders = ('xyz', 'yzx', 'zxy')

    def block(fixed, free):
        val = dict(fixed)
        val.update(free)
        return val['z'] * FOUR + val['y'] * TWO + val['x']

    slab_copy = pltpu.make_async_copy(slab_ref.at[pl.ds(row0, e_ref.shape[ZERO])], e_ref, s_slab)
    slab_copy.start()
    base = (tp * ndp + dp) * live + row0
    ntok = h_ref.shape[ZERO] // tt
    nrow = e_ref.shape[ZERO] // sub

    def tile(i, carry):
        at = pl.multiple_of((i % nrow) * sub, sub)
        t = i // nrow
        h = h_ref[pl.ds(pl.multiple_of(t * tt, tt), tt), :]
        row = lax.broadcasted_iota(jnp.int32, (sub, ONE), ZERO) + (base + at)
        p = jnp.exp(dot(e_ref[pl.ds(at, sub), :], h, NT) - lse_ref[t])
        d = jnp.where(row == lab_ref[t], p - 1.0, p).astype(bf16)
        g_ref[pl.ds(at, sub), :] += dot(d, h, NN)
        return carry

    def head_rows(first, last):
        lax.fori_loop(first * ntok * nrow // 16, last * ntok * nrow // 16, tile, ZERO)

    recvs = (r_one, r_two, r_last)
    flight = {}

    def send(k, step):
        order = orders[k]
        fixed = {d: bit[d] for d in order[:step]}
        fixed[order[step]] = ONE - bit[order[step]]
        rest = order[step + ONE:]
        for la in range(nl):
            for i in range(TWO ** len(rest)):
                free = {d: (i >> j) % TWO for j, d in enumerate(rest)}
                c = remote(acc.at[k, la, block(fixed, free)], recvs[step].at[k, la, i], s_ring.at[step, k, la, i], r_ring.at[step, k, la, i], near[order[step]])
                c.start()
                flight[k, step, la, i] = c

    def take(k, step):
        order = orders[k]
        fixed = {d: bit[d] for d in order[:step + ONE]}
        rest = order[step + ONE:]
        for la in range(nl):
            for i in range(TWO ** len(rest)):
                flight[k, step, la, i].wait_recv()
                free = {d: (i >> j) % TWO for j, d in enumerate(rest)}
                at = block(fixed, free)
                acc[k, la, at] = acc[k, la, at] + recvs[step][k, la, i]

    g_ref[:] = jnp.zeros_like(g_ref)
    slab_copy.wait()
    head_rows(ZERO, FOUR)
    for k in range(THREE):
        for la in range(nl):
            own[k, la].wait()
            over_core[k, la].wait_recv()
            acc[k, la] = acc[k, la] + r_core[k, la]
        if k:
            send(k - ONE, ZERO)
    send(TWO, ZERO)
    head_rows(FOUR, 12)
    for step in range(ONE, THREE):
        for k in range(THREE):
            take(k, step - ONE)
            if k:
                send(k - ONE, step)
        send(TWO, step)
        head_rows(FOUR * step + 8, 16)
    g_ref[:] *= inv
    for k in range(THREE):
        take(k, TWO)
        at = block(bit, {})
        for la in range(nl):
            out[la, k * third:(k + ONE) * third, :] = acc[k, la, at]
    for c in list(over_core.values()) + list(flight.values()):
        c.wait_send()
    for c in small:
        c.wait()
    total = slots[ZERO]
    for k in range(ONE, n):
        total = total + slots[k]
    small_out[:] = total


def grad_sum(packs, x, slab, row0, nrow, h, lse, lab, live, inv, ntp, ndp, cid):
    nl, rows = len(packs), packs[ZERO].shape[TWO]
    dim = slab.shape[ONE]
    third = rows // THREE
    vm, hbm = pl.BlockSpec(memory_space=pltpu.VMEM), pl.BlockSpec(memory_space=pl.ANY)
    n = ntp * ndp
    dma, buf = pltpu.SemaphoreType.DMA, pltpu.VMEM
    return pl.pallas_call(
        functools.partial(grad_sum_kernel, nl=nl, third=third, ntp=ntp, ndp=ndp, live=live, tt=lse.shape[TWO], sub=nrow // 5, inv=inv, row0=row0),
        in_specs=[hbm] * nl + [vm, hbm, vm, vm, vm], out_specs=[vm, vm, vm],
        out_shape=[jax.ShapeDtypeStruct((nl, rows, WIDE), f32), jax.ShapeDtypeStruct(x.shape, f32), jax.ShapeDtypeStruct((nrow, dim), f32)],
        scratch_shapes=[buf((THREE, nl, 8, third, WIDE), f32), buf((THREE, nl, 8, third, WIDE), f32), buf((THREE, nl, FOUR, third, WIDE), f32),
                        buf((THREE, nl, TWO, third, WIDE), f32), buf((THREE, nl, ONE, third, WIDE), f32), buf((n,) + x.shape, f32),
                        dma((THREE, nl)), dma((THREE, nl)), dma((THREE, nl)), dma((THREE, THREE, nl, FOUR)), dma((THREE, THREE, nl, FOUR)), dma((n - ONE,)), dma((n - ONE,)), buf((nrow, dim), bf16), dma],
        compiler_params=pltpu.CompilerParams(collective_id=cid, has_side_effects=True, vmem_limit_bytes=63 * MIB),
        cost_estimate=COST)(*packs, x, slab, h, lse, lab)


def adam_kernel(where_ref, clip_ref, tok_ref, *refs, n):
    g_refs, (p_ref, m_ref, v_ref), (po, mo, vo, bo, tok) = refs[:n], refs[n:n + THREE], refs[-5:]
    for k in range(n):
        @pl.when(pl.program_id(ZERO) == k)
        def _(k=k):
            new, mom, vel = adam_update(p_ref[:], g_refs[k][:] * clip_ref[ZERO], m_ref[:], v_ref[:], True)
            tok[:] = new[:8, :LANES]
            po[:] = new
            mo[:] = mom
            vo[:] = vel
            bo[:] = new.astype(bf16)


def adam_rows(where, clip, tok, grads, master, mom, vel, prev, nblk):
    n, (rows, wide) = len(grads), grads[ZERO].shape
    r = rows // nblk
    blk = pl.BlockSpec((r, wide), lambda i, j, w: (w[ZERO, i] + j, w[ONE, i]))
    anyspec = pl.BlockSpec(memory_space=pl.ANY)
    ins = [where, clip, tok] + list(grads) + [master, mom, vel]
    hold = lambda k: (lambda i, j, w: (jnp.where(i == k, j, jnp.where(i < k, ZERO, nblk - ONE)), ZERO))
    in_specs = [pl.BlockSpec(memory_space=pltpu.SMEM), anyspec] + [pl.BlockSpec((r, wide), hold(k)) for k in range(n)] + [blk] * THREE
    aliases = {}
    if prev is not None:
        aliases = {len(ins) + i: i for i in range(FOUR)}
        ins += list(prev)
        in_specs += [anyspec] * FOUR
    full = jax.ShapeDtypeStruct(master.shape, f32)
    return pl.pallas_call(
        functools.partial(adam_kernel, n=n),
        grid_spec=pltpu.PrefetchScalarGridSpec(num_scalar_prefetch=ONE, grid=(n, nblk), in_specs=in_specs, out_specs=[blk] * FOUR + [pl.BlockSpec((8, LANES), lambda i, j, w: (ZERO, ZERO))]),
        out_shape=[full, full, full, jax.ShapeDtypeStruct(master.shape, bf16), jax.ShapeDtypeStruct((8, LANES), f32)],
        input_output_aliases=aliases,
        compiler_params=pltpu.CompilerParams(dimension_semantics=("arbitrary", "arbitrary"), vmem_limit_bytes=48 * MIB),
        cost_estimate=COST,
        name="adam_rows")(*ins)


def solution(mesh):
    ntp, ndp = mesh.shape['tp'], mesh.shape['dp']
    ndev = ntp * ndp
    SWAP = {'z': [(i, ONE - i) for i in range(TWO)], 'core': [(i, i ^ ONE) for i in range(ndp)], 'x': [(i, i ^ TWO) for i in range(ndp)], 'y': [(i, i ^ FOUR) for i in range(ndp)]}

    def swap_on(val, axis):
        if axis == 'xz':
            return lax.ppermute(val, ('tp', 'dp'), [(i, i ^ (ndp + TWO)) for i in range(ndev)])
        return lax.ppermute(val, 'tp' if axis == 'z' else 'dp', SWAP[axis])

    def device_step(tokens, labels, *state):
        masters, moms, vels = state[ZERO:8], state[8:16], state[16:24]
        embedding, vec_params, w_qkv, b_qkv, w_out, w_up, b_up, w_down = masters
        z, dp = lax.axis_index('tp'), lax.axis_index('dp')
        yb, xb, cb = dp // FOUR, (dp // TWO) % TWO, dp % TWO
        vocab_loc, dim = embedding.shape
        layers = w_qkv.shape[ZERO]
        seq = tokens.shape[ONE]
        heads_loc, hd = b_qkv.shape[ONE], b_qkv.shape[TWO] // THREE
        heads = heads_loc * ntp
        n_total = seq * ndev
        vocab_base = z * vocab_loc
        live = vocab_loc // ndp
        half = -(-live // LANES) * LANES
        pick = lambda arr, i: lax.dynamic_index_in_dim(arr, i, ZERO, keepdims=False)

        def rows_of(ids):
            local = ids - vocab_base
            ok = (local >= ZERO) & (local < vocab_loc)
            return jnp.where(ok[:, None], gather_rows(jnp.where(ok, local, jnp.where(local < ZERO, local + vocab_loc, local - vocab_loc)), embedding), 0.0)

        tok_own, tok_oth = pick(tokens, z), pick(tokens, ONE - z)
        lab_own, lab_oth = pick(labels, z), pick(labels, ONE - z)
        ws = (w_down, w_up, w_out, w_qkv)
        dp1 = dp.reshape(ONE)
        got = [swap_on(pack_share(dp1, ws, layer, ndp), 'z') for layer in range(layers)]
        rows_out = rows_of(tok_oth)
        other = [lax.all_gather(g, 'dp', axis=ZERO, tiled=False) for g in got]
        row_got = swap_on(rows_out, 'z')
        row_own = rows_of(tok_own)
        lab_oth_rows, lab_own_rows = rows_of(lab_oth), rows_of(lab_own)
        bias_oth = swap_on(jnp.concatenate([b_qkv.reshape(layers, -ONE), b_up], axis=ONE), 'z')
        slab = make_slab(jnp.stack([dp, dp ^ FOUR]), embedding, live, half)

        ids = jnp.stack([jnp.stack([tok_own, tok_oth]), jnp.stack([lab_own, lab_oth])])
        ids = jnp.stack([ids, swap_on(ids, 'core')])
        ids = jnp.stack([ids, swap_on(ids, 'x')])
        ids_y = jnp.stack([ids, swap_on(ids, 'y')])
        tok_all = ids_y[:, :, :, ZERO]
        for axis, bit in ((ZERO, yb), (ONE, xb), (TWO, cb), (THREE, z)):
            tok_all = jnp.where(bit == ONE, jnp.flip(tok_all, axis), tok_all)
        tok_all = jnp.transpose(tok_all, (THREE, ZERO, ONE, TWO, FOUR)).reshape(-ONE)
        depth = ONE << (live - ONE).bit_length()
        row_id = tok_all - (vocab_base + dp * live)
        mine = (row_id >= ZERO) & (row_id < live)
        key = jnp.where(mine, jnp.arange(tok_all.shape[ZERO], dtype=jnp.int32) * depth + row_id, jnp.iinfo(jnp.int32).max)
        key = lax.sort(key, is_stable=False)
        key = jnp.where(key == jnp.iinfo(jnp.int32).max, live, key)
        count = jnp.sum(mine.astype(jnp.int32)).reshape(ONE)

        early = (row_own, lab_oth_rows, lab_own_rows, slab, key, count, ids, bias_oth, other[ZERO])
        row_own, lab_oth_rows, lab_own_rows, slab, key, count, ids, bias_oth, other[ZERO] = lax.optimization_barrier(early)
        joined = [join_halves(other[ZERO], ws, ZERO, hd)]
        row_got, joined[ZERO] = lax.optimization_barrier((row_got, joined[ZERO]))
        x_embed = row_got + row_own
        x_label = swap_on(lab_oth_rows, 'z') + lab_own_rows

        nbq = heads_loc * THREE * hd
        by_kind = lambda w: w.reshape(w.shape[:-ONE] + (heads_loc, THREE, hd)).swapaxes(-THREE, -TWO).reshape(w.shape[:-ONE] + (THREE, heads_loc * hd))

        def biases(layer):
            bq = jnp.concatenate([by_kind(b_qkv[layer].reshape(-ONE)), by_kind(bias_oth[layer, :nbq])], axis=-ONE).reshape(-ONE)
            return bq, jnp.concatenate([b_up[layer], bias_oth[layer, nbq:]], axis=ZERO)

        weights = []
        slope_all = jnp.array(alibi_slopes(heads), dtype=f32).reshape(ntp, heads_loc)
        slopes = jnp.concatenate([pick(slope_all, z), pick(slope_all, ONE - z)])

        ablk = min(512, seq)
        resid, ln_zero_vjp = jax.vjp(layer_norm, x_embed, vec_params[ZERO], vec_params[ONE])
        saved = []
        for layer in range(layers):
            k = TWO + 6 * layer
            wd, wu, wo, wq = joined[layer]
            bq, bu = biases(layer)
            weights.append((wq, bq, wo, wu, bu, wd))
            normed_one, ln_one_vjp = jax.vjp(layer_norm, resid, vec_params[k], vec_params[k + ONE])
            act_in = normed_one.astype(bf16)
            qkv = (dot(act_in, wq, NN) + bq).astype(bf16)
            context = attn_fwd(qkv, slopes, hd, ablk)
            if layer + ONE < layers:
                context, other[layer + ONE] = lax.optimization_barrier((context, other[layer + ONE]))
                joined.append(join_halves(other[layer + ONE], ws, layer + ONE, hd))
            mid = resid + (dot(context, wo, NN) + vec_params[k + TWO])
            normed_two, ln_two_vjp = jax.vjp(layer_norm, mid, vec_params[k + THREE], vec_params[k + FOUR])
            mlp_in = normed_two.astype(bf16)
            act_out, gelu_vjp = jax.vjp(gelu_tanh, dot(mlp_in, wu, NN) + bu)
            hidden = act_out.astype(bf16)
            resid = mid + dot(hidden, wd, NN) + vec_params[k + 5]
            saved.append((ln_one_vjp, act_in, qkv, context, ln_two_vjp, mlp_in, gelu_vjp, hidden))

        fin = TWO + 6 * layers
        normed_fin, ln_fin_vjp = jax.vjp(layer_norm, resid, vec_params[fin], vec_params[fin + ONE])
        t = seq // TWO
        core_own = swap_on(normed_fin, 'core')
        first, core_own = lax.optimization_barrier((normed_fin, core_own))
        a_own, b_own = first[:t], first[t:]
        a_x, a_z = swap_on(a_own, 'x'), swap_on(a_own, 'z')
        b_x, b_z = swap_on(b_own, 'x'), swap_on(b_own, 'z')
        groups = [[(first, ZERO), (first, ONE)], [(a_x, ZERO), (a_z, ZERO)], [(b_x, ZERO), (b_z, ZERO)], None, []]
        masks = [[(ZERO, ZERO, ZERO), (ZERO, ZERO, ONE)], [(ONE, ZERO, ZERO), (ZERO, ONE, ZERO)], [(ONE, ZERO, ONE), (ZERO, ONE, ONE)], [(ONE, ONE, ZERO), (ONE, ONE, ONE)]]
        hb, pos, self_sum, core_sum, tops, totals = None, ZERO, [], [], [], []
        from_core = []
        where_piece = {}
        for i, group in enumerate(groups):
            res = head_fwd(slab, group, from_core, hb, pos, 16, t, live, 1280)
            hb, top, total = res[-ONE], res[-THREE], res[-TWO]
            if i == ONE:
                a_far, b_far, top = lax.optimization_barrier((a_own, b_own, top))
                groups[THREE] = [(swap_on(a_far, 'xz'), ZERO), (swap_on(b_far, 'xz'), ZERO)]
            tops.append(top)
            totals.append(total)
            for side, names in ((ZERO, masks[i] if group else ()), (ONE, masks[i - ONE] if from_core else ())):
                for nm in names:
                    where_piece[nm + (side,)] = pos
                    pos += ONE
            if group:
                self_sum.append(res[ZERO])
            if from_core:
                core_sum.append(swap_on(res[-FOUR], 'core'))
            if i == ZERO:
                from_core = [(core_own, ZERO), (core_own, ONE)]
            elif group:
                moved = [arr for arr, _ in group]
                *moved, tops[i - ONE] = lax.optimization_barrier((*moved, tops[i - ONE]))
                from_core = [(swap_on(arr, 'core'), ZERO) for arr in moved]
        cube = [(x, zz, c, h) for x in range(TWO) for zz in range(TWO) for c in range(TWO) for h in range(TWO)]
        back = [ZERO] * 16
        for i, (x, zz, c, h) in enumerate(cube):
            back[where_piece[(x, zz, h, c)]] = i
        to_cube = lambda v: jnp.stack([v[where_piece[(x, zz, h, c)]] for x, zz, c, h in cube])
        from_cube = lambda v: jnp.stack([v[back[i]] for i in range(16)])
        m_loc = jnp.concatenate(tops).reshape(16, t)
        s_loc = jnp.concatenate(totals).reshape(16, t)
        stat = jnp.stack([to_cube(m_loc), to_cube(s_loc)]).reshape(TWO, TWO, TWO, TWO, TWO, t)
        m_core = None
        for axis, name in ((THREE, 'core'), (ONE, 'x'), (TWO, 'z')):
            got = jnp.flip(swap_on(stat, name), axis)
            if m_core is None:
                m_core = from_cube(got[ZERO].reshape(16, t))
            top = jnp.maximum(stat[ZERO], got[ZERO])
            stat = jnp.stack([top, stat[ONE] * jnp.exp(stat[ZERO] - top) + got[ONE] * jnp.exp(got[ZERO] - top)])
        stat = stat.reshape(TWO, 16, t)
        lse_cube = stat[ZERO] + jnp.log(stat[ONE])
        lse = from_cube(lse_cube)
        lab = from_cube(jnp.transpose(ids[:, :, ONE], (ZERO, TWO, ONE, THREE)).reshape(16, t))

        inv_n = 1.0 / n_total
        w_self, w_core = jnp.exp(m_loc - lse) * inv_n, jnp.exp(m_core - lse) * inv_n
        spread = lambda w, names, side: jnp.concatenate([w[where_piece[nm + (side,)]] for nm in names]).reshape(-ONE, ONE)
        reduced = [mine * spread(w_self, names, ZERO) + theirs * spread(w_core, names, ZERO) for mine, theirs, names in zip(self_sum, core_sum, masks)]
        r_own, r_one, r_two, r_far = reduced

        tt = 2048
        lse_t, lab_t = lse.reshape(-ONE, ONE, tt), lab.reshape(-ONE, ONE, tt)
        vb = half // TWO
        grad_args = dict(vb=vb, tt=tt, sub=vb // 5, inv=inv_n)
        base_own = (vocab_base + dp * live).reshape(ONE)
        base_oth = (vocab_base + (dp ^ FOUR) * live).reshape(ONE)
        hb0, r_own, r_one, r_two, r_far = lax.optimization_barrier((hb, r_own, r_one, r_two, r_far))
        got_z, got_far_z = swap_on(r_one[t:], 'z'), swap_on(r_far[:t], 'z')
        got_x, got_far_x = swap_on(r_two[:t], 'x'), swap_on(r_far[t:], 'x')
        g_send = head_grad(base_oth, slab, TWO, ONE, hb0, lse_t, lab_t, **grad_args)
        g_sent = [swap_on(g_send, 'y')]
        hb1, g_send, got_z, got_far_z, got_x, got_far_x = lax.optimization_barrier((hb0, g_send, got_z, got_far_z, got_x, got_far_x))
        a_sum, a_x_sum = r_own[:t] + got_z, r_one[:t] + got_far_z
        b_sum, b_z_sum = r_own[t:] + got_x, r_two[t:] + got_far_x
        hb1, a_x_sum, b_z_sum = lax.optimization_barrier((hb1, a_x_sum, b_z_sum))
        a_last, b_last = swap_on(a_x_sum, 'x'), swap_on(b_z_sum, 'z')
        g_send = head_grad(base_oth + vb, slab, THREE, ONE, hb1, lse_t, lab_t, **grad_args)
        g_sent.append(swap_on(g_send, 'y'))
        a_last, b_last, x_label = lax.optimization_barrier((a_last, b_last, x_label))
        d_head = jnp.concatenate([a_sum + a_last, b_sum + b_last], axis=ZERO) - x_label * inv_n
        target = jnp.sum(normed_fin.astype(bf16).astype(f32) * x_label, axis=ONE)
        loss_sum = jnp.sum(lse_cube[ZERO:TWO].reshape(-ONE) - target)

        vec_grads = {}
        d_resid, vec_grads[fin], vec_grads[fin + ONE] = ln_fin_vjp(d_head)
        bias_grads, part = {}, {}
        z1 = z.reshape(ONE)
        to_heads = lambda g: g.reshape(THREE, heads_loc, hd).swapaxes(ZERO, ONE).reshape(-ONE)
        rows_mlp = (w_down.shape[ONE] * w_down.shape[TWO] + w_up.shape[ONE] * w_up.shape[TWO]) // (ndp * WIDE)
        rows_attn = (w_out.shape[ONE] * w_out.shape[TWO] + w_qkv.shape[ONE] * w_qkv.shape[TWO]) // (ndp * WIDE)
        narrow = tt // TWO

        def sum_layer(layer, x, h, cid):
            pack = part[layer].reshape(ndev // TWO, TWO, -ONE, WIDE)
            return grad_sum([pack], x, slab, layer * vb, vb, h, lse.reshape(-ONE, ONE, narrow), lab.reshape(-ONE, ONE, narrow), live, inv_n, ntp, ndp, cid)

        for layer in reversed(range(layers)):
            ln_one_vjp, act_in, qkv, context, ln_two_vjp, mlp_in, gelu_vjp, hidden = saved[layer]
            wq, bq, wo, wu, bu, wd = weights[layer]
            k = TWO + 6 * layer
            vec_grads[k + 5] = jnp.sum(d_resid, axis=ZERO)
            d_out = d_resid.astype(bf16)
            d_pre = gelu_vjp(dot(d_out, wd, NT))[ZERO]
            g_bup = jnp.sum(d_pre, axis=ZERO)
            d_pre_b = d_pre.astype(bf16)
            g_pack = wgrad(wgrad_mlp_kernel, z1, (ONE, ZERO, ZERO, ONE), (hidden, d_out, mlp_in, d_pre_b), ndp, rows_mlp, ZERO, rows_mlp + rows_attn, None)
            d_mid_ln, vec_grads[k + THREE], vec_grads[k + FOUR] = ln_two_vjp(dot(d_pre_b, wu, NT))
            d_mid = d_resid + d_mid_ln
            vec_grads[k + TWO] = jnp.sum(d_mid, axis=ZERO)
            d_attn = d_mid.astype(bf16)
            d_context = dot(d_attn, wo, NT).astype(bf16)
            d_q, d_k, d_v, d_b = attn_bwd(qkv, d_context, slopes, hd, ablk)
            d_q, g_sent[layers - ONE - layer] = lax.optimization_barrier((d_q, g_sent[layers - ONE - layer]))
            d_res_ln, vec_grads[k], vec_grads[k + ONE] = ln_one_vjp(dot(jnp.concatenate([d_q, d_k, d_v], axis=ONE), wq, NT))
            d_resid = d_mid + d_res_ln
            if layer == ZERO:
                d_embed, vec_grads[ZERO], vec_grads[ONE] = ln_zero_vjp(d_resid)
                d_embed, hb2 = lax.optimization_barrier((d_embed, hb1))
                d_all = lax.all_gather(d_embed.reshape(seq, dim // LANES, LANES), ('tp', 'dp'), axis=ZERO, tiled=True)
            part[layer] = wgrad(wgrad_attn_kernel, z1, (ONE, ZERO, ZERO, ONE, ONE, ONE), (context, d_attn, act_in, d_q, d_k, d_v), ndp, rows_attn, rows_mlp, rows_mlp + rows_attn, g_pack)
            if layer == ONE:
                piece_1, _, own_1 = sum_layer(ONE, jnp.zeros((8, LANES), f32), hb1, THREE)
                d_resid, piece_1 = lax.optimization_barrier((d_resid, piece_1))
            d_bias = d_b[:THREE].reshape(THREE, ntp, heads_loc * hd)
            bias_grads[layer] = (to_heads(d_bias[:, ZERO]), to_heads(d_bias[:, ONE]), g_bup[:b_up.shape[ONE]], g_bup[b_up.shape[ONE]:])

        vec_g = jnp.stack([vec_grads[row] for row in range(fin + TWO)])
        own_b = jnp.concatenate([jnp.concatenate([bias_grads[la][ZERO], bias_grads[la][TWO]]) for la in range(layers)])
        oth_b = jnp.concatenate([jnp.concatenate([bias_grads[la][ONE], bias_grads[la][THREE]]) for la in range(layers)])
        both = jnp.where(z == ZERO, jnp.stack([own_b, oth_b]), jnp.stack([oth_b, own_b]))
        small = jnp.concatenate([vec_g.reshape(-ONE), both.reshape(-ONE), jnp.full((1024,), 1.0 / 1024, f32) * loss_sum])
        piece_0, small, own_0 = sum_layer(ZERO, small.reshape(-ONE, LANES), hb2, ONE)
        pieces = jnp.concatenate([piece_0, piece_1], axis=ZERO)
        small, pieces = small.reshape(-ONE), pieces.reshape(-ONE, WIDE)
        d_all, pieces = lax.optimization_barrier((d_all, pieces))
        left, right, sq_emb = add_lookup_rows(count, key, d_all, [own_0, own_1], g_sent, live, depth)
        nvec, nb = vec_g.size, own_b.size
        g_vec = small[:nvec].reshape(vec_g.shape)
        b_all = small[nvec:nvec + TWO * nb].reshape(TWO, nb)
        g_bias = pick(b_all, z).reshape(layers, -ONE)
        loss = jnp.sum(small[nvec + TWO * nb:]) / n_total
        sq_small = jnp.sum(g_vec * g_vec) + jnp.sum(b_all * b_all)

        sq_here = jnp.sum(sq_emb) + jnp.sum(pieces * pieces)
        sq_total = small_sum(jnp.full((8, LANES), 1.0 / 1024, f32) * sq_here, ntp, ndp, TWO)
        clip_coef = jnp.minimum(1.0, CLIP_NORM / (jnp.sqrt(jnp.sum(sq_total) + sq_small) + 1e-6))

        g_layers = lax.all_gather(pieces, 'dp', axis=ZERO, tiled=False)
        order = (7, 5, FOUR, TWO)
        take = lambda st: [st[i] for i in order]
        res = adam_layers(clip_coef.reshape(ONE), g_layers, take(masters), take(moms), take(vels), layers, hd)
        g_bqkv = g_bias[:, :nbq].reshape(b_qkv.shape)
        small_grads = {ONE: g_vec, THREE: g_bqkv, 6: g_bias[:, nbq:]}

        left, right, clip_coef = lax.optimization_barrier((left, right, clip_coef))
        left_x, right_y = swap_on(left, 'x'), swap_on(right, 'y')
        left_y, right_x = swap_on(left, 'y'), swap_on(right, 'x')
        nblk, emb_new, clip1 = THREE, None, clip_coef.reshape(ONE)
        tok = jnp.zeros((8, LANES), f32)

        def update(pieces, prev, tok, first=ZERO, count=nblk):
            where = jnp.stack([jnp.stack([(dp ^ mask) * nblk + first for _, mask, _ in pieces]), jnp.array([col for _, _, col in pieces], jnp.int32)])
            *new, tok = adam_rows(where, clip1, tok, [g for g, _, _ in pieces], embedding, moms[ZERO], vels[ZERO], prev, count)
            return new, tok

        over = lambda pieces: [(swap_on(g, 'core'), mask + ONE, col) for g, mask, col in pieces]
        stage = [(left, ZERO, ZERO), (right, ZERO, ONE)]
        cross = over(stage)
        emb_new, tok = update(stage, None, tok)
        emb_new, tok = update(cross, emb_new, tok)
        left_x, right_y, tok = lax.optimization_barrier((left_x, right_y, tok))
        r = live // nblk
        far = [(swap_on(left_x[j * r:(j + ONE) * r], 'y'), swap_on(right_y[j * r:(j + ONE) * r], 'x')) for j in range(nblk)]
        stages = [([(left_x, TWO, ZERO), (right_y, FOUR, ONE)], ZERO, nblk), ([(left_y, FOUR, ZERO), (right_x, TWO, ONE)], ZERO, nblk)]
        stages += [([(fl, 6, ZERO), (fr, 6, ONE)], j, ONE) for j, (fl, fr) in enumerate(far)]
        for stage, first_blk, nb_here in stages:
            *got, tok = lax.optimization_barrier((*(g for g, _, _ in stage), tok))
            stage = [(g, mask, col) for g, (_, mask, col) in zip(got, stage)]
            cross = over(stage)
            emb_new, tok = update(stage, emb_new, tok, first_blk, nb_here)
            emb_new, tok = update(cross, emb_new, tok, first_blk, nb_here)

        updated = {ZERO: tuple(emb_new)}
        for i, slot in enumerate(order):
            updated[slot] = (res[i], res[FOUR + i], res[8 + i], res[12 + i])
        for slot, g in small_grads.items():
            new = adam_update(masters[slot], g * clip_coef, moms[slot], vels[slot], DECAYED[slot])
            updated[slot] = (*new, new[ZERO].astype(bf16))
        new_masters, new_moms, new_vels, new_bf16 = ([updated[slot][i] for slot in range(8)] for i in range(FOUR))
        return (loss, *new_masters, *new_moms, *new_vels, *new_bf16)

    data_spec = P('dp', None)
    return jax.shard_map(device_step, mesh=mesh, in_specs=(data_spec, data_spec) + PARAM_SPECS * THREE, out_specs=(P(),) + PARAM_SPECS * FOUR, check_vma=False)
```
